32 devices in a mesh: occ: 4 (over y, x), vir: 8 (over z, core).
Axes of the slice: x: 2, y: 2, z: 4, core: 2. Of those that a mesh axis runs over, the one named last changes fastest.
Arguments:
- b_factors: float32 [32, 256, 4096], P('occ', 'vir'), may hold values from -0.6 to 0.6
- occ_energy: float32 [32], replicated, may hold values from -2 to -0.3
- vir_energy: float32 [256], replicated, may hold values from 0.2 to 3
Outputs:
- gamma: float32 [32, 256, 4096], P('occ', 'vir')
The draws below stay inside these ranges and needn't reach their ends.
All inputs are finite; a program needn't handle non-finite values.
Results may differ from the reference program's by a relative error of at most 0.0003.
Values sent between devices are 32-bit elements; how exact they have to be, the bound alone decides.
A program may use at most 128 MiB of HBM per device.

```python
import jax
import jax.numpy as jnp
from jax import lax

P_SIZE = 4096
OCC_DEV = 8
VIR_DEV = 32
O = 32
V = 256
N_OCC = 4
N_VIR = 8


def steps_of(own_key, extent, pieces, smallest, top_value):
    loudness, own = 1.0, jax.random.fold_in(own_key, 6)
    for axis_at, blocks in pieces:
        steps = jnp.exp(jax.random.uniform(jax.random.fold_in(own, axis_at), (blocks,), jnp.float32, smallest / len(pieces), top_value / len(pieces)))
        loudness = loudness * jnp.repeat(steps, extent[axis_at] // blocks).reshape([-1 if axis == axis_at else 1 for axis in range(len(extent))])
    return loudness


def bell_draw(stream_key, dims, spread, bound, pieces=(), kind=jnp.bfloat16):
    values = spread * jax.random.normal(stream_key, dims, jnp.float32)
    if pieces:
        values = values * steps_of(stream_key, dims, pieces, -0.22, 0.18)
    return jnp.clip(values, -bound, bound).astype(kind)


def setup_inputs(seed: int = 0) -> dict:
    key_list = jax.random.split(jax.random.key(seed), 4)
    b_factors = bell_draw(key_list[0], (O, V, P_SIZE), 0.1, 0.6, ((0, 4), (1, 8)), jnp.float32)
    occ_energy = jnp.clip(jax.random.uniform(key_list[1], (O,), jnp.float32, -2.0, -0.3), -2.0, -0.3)
    vir_energy = jnp.clip(jax.random.uniform(key_list[2], (V,), jnp.float32, 0.2, 3.0), 0.2, 3.0)
    return {"b_factors": b_factors, "occ_energy": occ_energy, "vir_energy": vir_energy}


def reference(b_factors, occ_energy, vir_energy):
    rows = OCC_DEV * VIR_DEV
    width = b_factors.shape[2]
    blocks = b_factors.reshape(N_OCC, OCC_DEV, N_VIR, VIR_DEV, width).transpose(0, 2, 1, 3, 4).reshape(N_OCC, N_VIR, rows, width)
    gaps = (occ_energy[:, None] - vir_energy[None, :]).reshape(N_OCC, OCC_DEV, N_VIR, VIR_DEV).transpose(0, 2, 1, 3).reshape(N_OCC, N_VIR, rows)
    offsets = [(0, 0), (1, 0), (-1, 0), (0, 1), (0, -1)]
    high = lax.Precision.HIGHEST

    def one_block_row(index):
        mine = blocks[index]
        mine_gap = gaps[index]
        total = jnp.zeros_like(mine)
        for shift_occ, shift_vir in offsets:
            other_index = (index + shift_occ) % N_OCC
            other = jnp.roll(blocks[other_index], -shift_vir, axis=0)
            other_gap = jnp.roll(gaps[other_index], -shift_vir, axis=0)
            integral = jnp.einsum("vrp,vsp->vrs", mine, other, precision=high)
            amplitude = integral / (mine_gap[:, :, None] + other_gap[:, None, :])
            total = total + jnp.einsum("vrs,vsp->vrp", amplitude, other, precision=high)
        return total

    result = lax.map(one_block_row, jnp.arange(N_OCC, dtype=jnp.int32))
    return result.reshape(N_OCC, N_VIR, OCC_DEV, VIR_DEV, width).transpose(0, 2, 1, 3, 4).reshape(N_OCC * OCC_DEV, N_VIR * VIR_DEV, width)
```

```python
import functools

import jax
import jax.numpy as jnp
from jax import lax
from jax.experimental import pallas as pl
from jax.experimental.pallas import tpu as pltpu
from jax.sharding import PartitionSpec as P

MESH = pl.DeviceIdType.MESH
CHUNK = 256
AHEAD = 4
LAG = 2
TILE = 512


def split(value):
    high = value.astype(jnp.bfloat16)
    low = (value - high.astype(jnp.float32)).astype(jnp.bfloat16)
    return high, low


def product(a, b, contract):
    dims = ((contract[:1], contract[1:]), ((), ()))
    dot = functools.partial(lax.dot_general, dimension_numbers=dims, preferred_element_type=jnp.float32)
    (a_high, a_low), (b_high, b_low) = a, b
    return dot(a_high, b_high) + (dot(a_high, b_low) + dot(a_low, b_high))


def kernel(
    occ_count, vir_count, occ_block, vir_block,
    occ_ref, vir_ref, b_ref, out_ref,
    own, near, far, up, down, own_high, own_low, total, sums,
    own_sem, out_sem, near_send, near_recv, far_send, far_recv, up_send, up_recv, down_send, down_recv,
):
    rows, width = b_ref.shape
    chunks = width // CHUNK
    tiles = width // TILE
    o = lax.axis_index("occ")
    v = lax.axis_index("vir")
    step = 1 - 2 * lax.rem(o, 2)
    partner = o + step
    relay_to = lax.rem(o + 2 * step + occ_count, occ_count)
    relay_from = lax.rem(o - 2 * step + occ_count, occ_count)
    across = lax.rem(o - step + occ_count, occ_count)
    v_up = lax.rem(v + 1, vir_count)
    v_down = lax.rem(v + vir_count - 1, vir_count)

    def cols(k, size=CHUNK):
        return pl.ds(pl.multiple_of(k * size, size), size)

    def load(k):
        return pltpu.make_async_copy(b_ref.at[:, cols(k)], own.at[:, cols(k)], own_sem.at[k])

    def near_copy(k):
        return pltpu.make_async_remote_copy(
            b_ref.at[:, cols(k)], near.at[:, cols(k)], near_send.at[k], near_recv.at[k],
            device_id=(partner, v), device_id_type=MESH)

    def far_copy(k):
        return pltpu.make_async_remote_copy(
            near.at[:, cols(k)], far.at[:, cols(k)], far_send.at[k], far_recv.at[k],
            device_id=(relay_to, v), device_id_type=MESH)

    def up_copy(k):
        return pltpu.make_async_remote_copy(
            b_ref.at[:, cols(k)], down.at[:, cols(k)], up_send.at[k], down_recv.at[k],
            device_id=(o, v_up), device_id_type=MESH)

    def down_copy(k):
        return pltpu.make_async_remote_copy(
            b_ref.at[:, cols(k)], up.at[:, cols(k)], down_send.at[k], up_recv.at[k],
            device_id=(o, v_down), device_id_type=MESH)

    def send(k):
        near_copy(k).start()
        up_copy(k).start()
        down_copy(k).start()

    def every(count, body, first=0):
        def run(k, carry):
            body(k)
            return carry
        lax.fori_loop(first, count, run, 0)

    barrier = pltpu.get_barrier_semaphore()
    for device in ((partner, v), (relay_to, v), (relay_from, v), (o, v_up), (o, v_down)):
        pl.semaphore_signal(barrier, inc=1, device_id=device, device_id_type=MESH)
    every(chunks, lambda k: load(k).start())
    pl.semaphore_wait(barrier, 5)
    every(AHEAD, send)

    lane = lax.broadcasted_iota(jnp.int32, (8, rows), 1)
    inner = lane
    for i in range(1, occ_block):
        inner = inner - jnp.where(lane >= i * vir_block, vir_block, 0)

    def gap_row(occ_place, vir_place):
        occ_part = jnp.zeros((8, rows), jnp.float32)
        vir_part = jnp.zeros((8, rows), jnp.float32)
        for i in range(occ_block):
            occ_part = jnp.where(lane >= i * vir_block, occ_ref[occ_place * occ_block + i], occ_part)
        for a in range(vir_block):
            vir_part = jnp.where(inner == a, vir_ref[vir_place * vir_block + a], vir_part)
        return jnp.broadcast_to((occ_part - vir_part)[:1], (rows, rows))

    mine_gap = gap_row(o, v).T

    def gather(slot, block, k):
        a = (own_high[:, cols(k)], own_low[:, cols(k)])
        sums[slot] += product(a, split(block[:, cols(k)]), (1, 1))

    def amplitude(slot, occ_place, vir_place):
        return split(sums[slot] / (mine_gap + gap_row(occ_place, vir_place)))

    def spread(amp, block, fresh=False, last=False):
        def tile(t):
            here = cols(t, TILE)
            part = product(amp, split(block[:, here]), (1, 0))
            total[:, here] = part if fresh else total[:, here] + part
            if last:
                pltpu.make_async_copy(total.at[:, here], out_ref.at[:, here], out_sem.at[t]).start()
        every(tiles, tile)

    sums[...] = jnp.zeros_like(sums)

    def own_chunk(k):
        load(k).wait()
        high, low = split(own[:, cols(k)])
        own_high[:, cols(k)] = high
        own_low[:, cols(k)] = low
        gather(0, own, k)

    every(chunks, own_chunk)
    spread(amplitude(0, o, v), own, fresh=True)

    def lagged(k):
        up_copy(k).wait_send()
        down_copy(k).wait_send()
        near_copy(k).wait_send()
        down_copy(k).wait_recv()
        gather(2, up, k)
        up_copy(k).wait_recv()
        gather(3, down, k)

    def lagged_far(k):
        far_copy(k).wait()
        gather(4, far, k)

    def arrive(k):
        near_copy(k).wait_recv()
        far_copy(k).start()

        @pl.when(k + AHEAD < chunks)
        def _():
            send(k + AHEAD)

        gather(1, near, k)

        @pl.when(k >= LAG)
        def _():
            lagged(k - LAG)
            lagged_far(k - LAG)

    every(chunks, arrive)
    spread(amplitude(1, partner, v), near)
    every(chunks, lagged, chunks - LAG)
    spread(amplitude(2, o, v_up), up)
    spread(amplitude(3, o, v_down), down)
    every(chunks, lagged_far, chunks - LAG)
    spread(amplitude(4, across, v), far, last=True)

    def stored(t):
        here = cols(t, TILE)
        pltpu.make_async_copy(total.at[:, here], out_ref.at[:, here], out_sem.at[t]).wait()

    every(tiles, stored)


def local(b_factors, occ_energy, vir_energy):
    occ_block, vir_block, width = b_factors.shape
    occ_count = lax.axis_size("occ")
    vir_count = lax.axis_size("vir")
    rows = occ_block * vir_block
    chunks, tiles = width // CHUNK, width // TILE
    block = pltpu.VMEM((rows, width), jnp.float32)
    half = pltpu.VMEM((rows, width), jnp.bfloat16)
    sems = [pltpu.SemaphoreType.DMA((count,)) for count in [chunks, tiles] + [chunks] * 8]
    out = pl.pallas_call(
        functools.partial(kernel, occ_count, vir_count, occ_block, vir_block),
        out_shape=jax.ShapeDtypeStruct((rows, width), jnp.float32),
        in_specs=[
            pl.BlockSpec(memory_space=pltpu.SMEM),
            pl.BlockSpec(memory_space=pltpu.SMEM),
            pl.BlockSpec(memory_space=pl.ANY),
        ],
        out_specs=pl.BlockSpec(memory_space=pl.ANY),
        scratch_shapes=[block] * 5 + [half, half, block, pltpu.VMEM((5, rows, rows), jnp.float32)] + sems,
        compiler_params=pltpu.CompilerParams(
            collective_id=0, has_side_effects=True, vmem_limit_bytes=60 * 2**20),
    )(occ_energy, vir_energy, b_factors.reshape(rows, width))
    return out.reshape(occ_block, vir_block, width)


def solution(mesh):
    in_specs = (P("occ", "vir", None), P(), P())
    out_specs = P("occ", "vir", None)
    return jax.shard_map(local, mesh=mesh, in_specs=in_specs, out_specs=out_specs, check_vma=False)
```

```python
import functools

import jax
import jax.numpy as jnp
from jax import lax
from jax.experimental import pallas as pl
from jax.experimental.pallas import tpu as pltpu
from jax.sharding import PartitionSpec as P

MESH = pl.DeviceIdType.MESH
CHUNK = 512
AHEAD = 4
LAG = 2
STREAMS = 4


def split(value):
    high = value.astype(jnp.bfloat16)
    low = (value - high.astype(jnp.float32)).astype(jnp.bfloat16)
    return high, low


def product(a, b, contract):
    dims = ((contract[:1], contract[1:]), ((), ()))
    dot = functools.partial(lax.dot_general, dimension_numbers=dims, preferred_element_type=jnp.float32)
    (a_high, a_low), (b_high, b_low) = a, b
    return dot(a_high, b_high) + (dot(a_high, b_low) + dot(a_low, b_high))


def cols(k):
    return pl.ds(pl.multiple_of(k * CHUNK, CHUNK), CHUNK)


def every(count, body, first=0):
    def run(k, carry):
        body(k)
        return carry
    lax.fori_loop(first, count, run, 0)


def kernel(
    occ_count, vir_count, occ_block, vir_block,
    occ_ref, vir_ref, b_ref, total, land, amp_high, amp_low,
    own, own_high, own_low, sums, mine_gap, vir_row,
    own_sem, near_send, near_recv, far_send, far_recv, inner_send, inner_recv, outer_send, outer_recv,
):
    rows, width = b_ref.shape
    piece = rows // STREAMS
    occ_piece = occ_block // STREAMS
    chunks = width // CHUNK
    steps = STREAMS * chunks
    o = lax.axis_index("occ")
    v = lax.axis_index("vir")
    step = 1 - 2 * lax.rem(o, 2)
    partner = o + step
    relay_to = lax.rem(o + 2 * step + occ_count, occ_count)
    relay_from = lax.rem(o - 2 * step + occ_count, occ_count)
    across = lax.rem(o - step + occ_count, occ_count)
    turn = 1 - 2 * lax.rem(v, 2)
    v_inner = v + turn
    v_outer = lax.rem(v - turn + vir_count, vir_count)
    sources = ((partner, v), (o, v_inner), (o, v_outer), (across, v))

    def sent(k):
        return b_ref.at[pl.ds(pl.multiple_of(k // chunks * piece, piece), piece), cols(k % chunks)]

    def landed(k, stream):
        return land.at[k // chunks, pl.ds(stream * piece, piece), cols(k % chunks)]

    def remote(k, source, stream, send_sem, recv_sem, device):
        return pltpu.make_async_remote_copy(
            source, landed(k, stream), send_sem.at[k], recv_sem.at[k], device_id=device, device_id_type=MESH)

    def load(k):
        return pltpu.make_async_copy(b_ref.at[:, cols(k)], own.at[:, cols(k)], own_sem.at[k])

    def near_copy(k):
        return remote(k, sent(k), 0, near_send, near_recv, (partner, v))

    def inner_copy(k):
        return remote(k, sent(k), 1, inner_send, inner_recv, (o, v_inner))

    def outer_copy(k):
        return remote(k, sent(k), 2, outer_send, outer_recv, (o, v_outer))

    def far_copy(k):
        return remote(k, landed(k, 0), 3, far_send, far_recv, (relay_to, v))

    def send(k):
        near_copy(k).start()
        outer_copy(k).start()
        inner_copy(k).start()

    barrier = pltpu.get_barrier_semaphore()
    for device in ((partner, v), (relay_to, v), (relay_from, v), (o, v_inner), (o, v_outer)):
        pl.semaphore_signal(barrier, inc=1, device_id=device, device_id_type=MESH)
    pl.semaphore_wait(barrier, 5)
    every(AHEAD, send)
    every(chunks, lambda k: load(k).start())

    lane = lax.broadcasted_iota(jnp.int32, (8, rows), 1)
    within = lane
    for i in range(1, occ_block):
        within = within - jnp.where(lane >= i * vir_block, vir_block, 0)

    def vir_values(blocks):
        values = jnp.zeros((8, rows), jnp.float32)
        for stream, block in enumerate(blocks):
            part = values
            for a in range(vir_block):
                part = jnp.where(within == a, vir_ref[block * vir_block + a], part)
            values = jnp.where(lane >= stream * piece, part, values)
        return values

    def occ_values(places):
        values = jnp.zeros((8, rows), jnp.float32)
        for i, place in enumerate(places):
            values = jnp.where(lane >= i * vir_block, occ_ref[place], values)
        return values

    def whole(row):
        return jnp.broadcast_to(row[:1], (rows, rows))

    own_row = occ_values([o * occ_block + i for i in range(occ_block)]) - vir_values([v])
    mine_gap[...] = whole(own_row).T
    vir_row[...] = vir_values([block for _, block in sources])

    def gather(block, k):
        a = (own_high[:, cols(k)], own_low[:, cols(k)])
        sums[...] += product(a, split(block), (1, 1))

    def amplitude(row):
        amp_high[...], amp_low[...] = split(sums[...] / (mine_gap[...] + whole(row)))
        sums[...] = jnp.zeros_like(sums)

    def spread(block):
        return product((amp_high[...], amp_low[...]), split(block), (1, 0))

    sums[...] = jnp.zeros_like(sums)

    def own_chunk(k):
        load(k).wait()
        high, low = split(own[:, cols(k)])
        own_high[:, cols(k)] = high
        own_low[:, cols(k)] = low
        gather(own[:, cols(k)], k)

    every(chunks, own_chunk)
    amplitude(own_row)

    def own_spread(k):
        total[:, cols(k)] = spread(own[:, cols(k)])

    def read(k):
        phase, here = k // chunks, k % chunks
        near_copy(k).wait_send()
        inner_copy(k).wait()
        outer_copy(k).wait()
        far_copy(k).wait()
        gather(land[phase, :, cols(here)], here)

        @pl.when(phase == 0)
        def _():
            own_spread(here)

        @pl.when(phase > 0)
        def _():
            total[:, cols(here)] += spread(land[jnp.maximum(phase - 1, 0), :, cols(here)])

        @pl.when(here == chunks - 1)
        def _():
            places = [
                block * occ_block + phase * occ_piece + i for block, _ in sources for i in range(occ_piece)]
            amplitude(occ_values(places) - vir_row[...])

    def arrive(k):
        near_copy(k).wait_recv()
        far_copy(k).start()

        @pl.when(k + AHEAD < steps)
        def _():
            send(k + AHEAD)

        @pl.when(k >= LAG)
        def _():
            read(k - LAG)

    every(steps, arrive)
    every(steps, read, steps - LAG)


def finish(total, land, amp_high, amp_low, out_ref, done, out_sem):
    amp = (amp_high[...], amp_low[...])
    chunks = total.shape[1] // CHUNK

    def store(k):
        return pltpu.make_async_copy(done.at[:, cols(k)], out_ref.at[:, cols(k)], out_sem.at[k])

    def tile(k):
        done[:, cols(k)] = total[:, cols(k)] + product(amp, split(land[STREAMS - 1, :, cols(k)]), (1, 0))
        store(k).start()

    every(chunks, tile)
    every(chunks, lambda k: store(k).wait())


def local(b_factors, occ_energy, vir_energy):
    occ_block, vir_block, width = b_factors.shape
    occ_count = lax.axis_size("occ")
    vir_count = lax.axis_size("vir")
    rows = occ_block * vir_block
    chunks = width // CHUNK
    steps = STREAMS * chunks
    block = pltpu.VMEM((rows, width), jnp.float32)
    half = pltpu.VMEM((rows, width), jnp.bfloat16)
    square = pltpu.VMEM((rows, rows), jnp.float32)
    vmem = pl.BlockSpec(memory_space=pltpu.VMEM)
    smem = pl.BlockSpec(memory_space=pltpu.SMEM)
    hbm = pl.BlockSpec(memory_space=pl.ANY)
    sems = [pltpu.SemaphoreType.DMA((count,)) for count in [chunks] + [steps] * 8]
    parts = pl.pallas_call(
        functools.partial(kernel, occ_count, vir_count, occ_block, vir_block),
        out_shape=[
            block,
            pltpu.VMEM((STREAMS, rows, width), jnp.float32),
            pltpu.VMEM((rows, rows), jnp.bfloat16),
            pltpu.VMEM((rows, rows), jnp.bfloat16),
        ],
        in_specs=[smem, smem, hbm],
        out_specs=[vmem] * 4,
        scratch_shapes=[block, half, half, square, square, pltpu.VMEM((8, rows), jnp.float32)] + sems,
        compiler_params=pltpu.CompilerParams(
            collective_id=0, has_side_effects=True, vmem_limit_bytes=42 * 2**20),
    )(occ_energy, vir_energy, b_factors.reshape(rows, width))
    out = pl.pallas_call(
        finish,
        out_shape=jax.ShapeDtypeStruct((rows, width), jnp.float32),
        in_specs=[vmem] * 4,
        out_specs=hbm,
        scratch_shapes=[block, pltpu.SemaphoreType.DMA((chunks,))],
        compiler_params=pltpu.CompilerParams(vmem_limit_bytes=10 * 2**20),
    )(*parts)
    return out.reshape(occ_block, vir_block, width)


def solution(mesh):
    in_specs = (P("occ", "vir", None), P(), P())
    out_specs = P("occ", "vir", None)
    return jax.shard_map(local, mesh=mesh, in_specs=in_specs, out_specs=out_specs, check_vma=False)
```
